32 devices in a mesh: win: 8 (over z, x), fsdp: 4 (over y, core).
Axes of the slice: x: 2, y: 2, z: 4, core: 2. Of those that a mesh axis runs over, the one named last changes fastest.
Arguments:
- queries: bfloat16 [8192, 2560], P(('win', 'fsdp')), may hold values from -5 to 5
- keys: bfloat16 [8192, 2560], P(('win', 'fsdp')), may hold values from -5 to 5
- values: bfloat16 [8192, 2560], P(('win', 'fsdp')), may hold values from -6 to 6
- stream: bfloat16 [8192, 5120], P(('win', 'fsdp')), may hold values from -0.59765625 to 0.59765625
- out_weight: bfloat16 [2560, 5120], P('fsdp', 'win'), may hold values from -0.125 to 0.125
- gate: float32 [5120], replicated, may hold values from 0.5 to 2
- head_shift: float32 [5120], replicated, may hold values from -3 to 3
- head_scale: float32 [5120], replicated, may hold values from 0.25 to 1.75
- head_weight: bfloat16 [5120, 64], replicated, may hold values from -0.078125 to 0.078125
- latents: float32 [128, 4096], P('win', 'fsdp'), may hold values from -6 to 6
- step_size: float32 [1], replicated, may hold values from 0.5 to 1
- intersections: int32 [8], replicated, may hold values from 1 to 4
- ramps: int32 [8, 4, 2], replicated, may hold values from 1 to 16
Outputs:
- blended: float32 [128, 4096], P('win', 'fsdp')
The draws below stay inside these ranges and needn't reach their ends.
All inputs are finite; a program needn't handle non-finite values.
Results may differ from the reference program's by a relative error of at most 0.0065.
Values may be sent and summed in bfloat16 or wider, within the bound.
A program may use at most 128 MiB of HBM per device.

```python
import math
import jax
import jax.numpy as jnp
from jax import lax

D = 5120
HEADS = 20
HD = 128
C = 64
P_SIZE = 64
FD = 4
FW = 16
TOKENS = 8192
FRAMES = 128
N_WIN = 8
N_FSDP = 4


def attention_pair(key):
    base = jax.random.fold_in(key, 7)
    first_key, second_key = jax.random.split(base, 2)
    total_rows = N_WIN * FD * N_FSDP * P_SIZE
    columns = HEADS * HD
    query_set = jnp.clip(jax.random.normal(first_key, (total_rows, columns), jnp.float32), -5.0, 5.0)
    key_set = jnp.clip(jax.random.normal(second_key, (total_rows, columns), jnp.float32), -5.0, 5.0)
    return (query_set.astype(jnp.bfloat16), key_set.astype(jnp.bfloat16))


def draw_queries(key, part):
    return attention_pair(key)[0]


def draw_keys(key, part):
    return attention_pair(key)[1]


def set_ends(entries, own_key, least, high):
    dims = entries.shape
    spot = [jax.random.randint(jax.random.fold_in(own_key, axis), (), 0, dims[axis]) for axis in range(len(dims))]
    entries = entries.at[tuple(spot)].set(least)
    longest = dims.index(max(dims))
    spot[longest] = (spot[longest] + 1) % dims[longest]
    return entries.at[tuple(spot)].set(high)


def level_of(stream_key, extent, cuts, least, top_value):
    def one(dim, shards_of):
        steps = jax.random.uniform(jax.random.fold_in(jax.random.fold_in(stream_key, 6), dim), (shards_of,), jnp.float32, least / len(cuts), top_value / len(cuts))
        return jnp.repeat(jnp.exp(steps), extent[dim] // shards_of).reshape((-1,) + (1,) * (len(extent) - dim - 1))

    factor_of = one(*cuts[0])
    for cut in cuts[1:]:
        factor_of = factor_of * one(*cut)
    return factor_of


def noise(own_key, dims, scale, reach, cuts=(), held_as=jnp.bfloat16):
    result = jax.random.normal(own_key, dims, jnp.float32) * scale
    if len(cuts) > 0:
        result = level_of(own_key, dims, cuts, -0.22, 0.18) * result
    return jnp.clip(result, min=-reach, max=reach).astype(held_as)


def setup_inputs(seed: int = 0) -> dict:
    key_list = jax.random.split(jax.random.key(seed), 14)
    queries = draw_queries(jax.random.fold_in(key_list[13], 71), 0)
    keys = draw_keys(jax.random.fold_in(key_list[13], 71), 0)
    values = noise(key_list[2], (TOKENS, HEADS * HD), 1.0, 6.0, ((0, 32),))
    stream = noise(key_list[3], (TOKENS, D), 0.1, 0.59765625, ((0, 32),))
    out_weight = noise(key_list[4], (HEADS * HD, D), (HEADS * HD) ** -0.5, 0.125, ((0, 4), (1, 8)))
    gate = jnp.clip(jax.random.uniform(key_list[5], (D,), jnp.float32, 0.5, 2.0), 0.5, 2.0)
    head_shift = noise(key_list[6], (D,), 0.5, 3.0, (), jnp.float32)
    head_scale = jnp.clip(1.0 + 0.15 * jax.random.normal(key_list[7], (D,), jnp.float32), 0.25, 1.75)
    head_weight = noise(key_list[8], (D, C), D ** -0.5, 0.078125)
    latents = noise(key_list[9], (FRAMES, P_SIZE * C), 1.0, 6.0, ((0, 8), (1, 4)), jnp.float32)
    step_size = jnp.clip(jax.random.uniform(key_list[10], (1,), jnp.float32, 0.5, 1.0), 0.5, 1.0)
    intersections = set_ends(jax.random.randint(key_list[11], (N_WIN,), 1, FD + 1), jax.random.fold_in(key_list[11], 1), 1, FD).astype(jnp.int32)
    ramps = set_ends(jax.random.randint(key_list[12], (N_WIN, FD, 2), 1, 17), jax.random.fold_in(key_list[12], 1), 1, 16).astype(jnp.int32)
    return {"queries": queries, "keys": keys, "values": values, "stream": stream, "out_weight": out_weight, "gate": gate, "head_shift": head_shift, "head_scale": head_scale, "head_weight": head_weight, "latents": latents, "step_size": step_size, "intersections": intersections, "ramps": ramps}


EPSILON = 0.001

def attend(window_parts):
    query_win, key_win, value_win = window_parts
    window_tokens = FW * P_SIZE
    query_h = query_win.reshape(window_tokens, HEADS, HD).astype(jnp.float32)
    key_h = key_win.reshape(window_tokens, HEADS, HD).astype(jnp.float32)
    value_h = value_win.reshape(window_tokens, HEADS, HD).astype(jnp.float32)
    scores = jnp.einsum('qhd,khd->hqk', query_h, key_h) * (1.0 / math.sqrt(HD))
    highest = lax.optimization_barrier(jnp.max(scores, axis=-1, keepdims=True))
    exponent = jnp.exp(scores - highest)
    denominator = lax.optimization_barrier(jnp.sum(exponent, axis=-1))
    probability = exponent.astype(jnp.bfloat16)
    probability = lax.optimization_barrier(probability).astype(jnp.float32)
    summed = jnp.einsum('hqk,khd->qhd', probability, value_h)
    attended = summed / jnp.transpose(denominator)[:, :, None]
    return attended.reshape(window_tokens, HEADS * HD).astype(jnp.bfloat16)

def reference(queries, keys, values, stream, out_weight, gate, head_shift, head_scale, head_weight, latents, step_size, intersections, ramps):
    window_tokens = FW * P_SIZE
    feat_width = HEADS * HD
    attended = lax.map(attend, (queries.reshape(N_WIN, window_tokens, feat_width), keys.reshape(N_WIN, window_tokens, feat_width), values.reshape(N_WIN, window_tokens, feat_width)))
    attended = attended.reshape(N_WIN * window_tokens, feat_width)
    projected = jnp.dot(attended, out_weight, preferred_element_type=jnp.float32)
    hidden = stream.astype(jnp.float32) + gate * projected
    centre = lax.optimization_barrier(jnp.mean(hidden, axis=-1, keepdims=True))
    centred = hidden - centre
    variance = lax.optimization_barrier(jnp.mean(centred * centred, axis=-1, keepdims=True))
    normed = centred / jnp.sqrt(variance + EPSILON)
    modulated = (normed * head_scale + head_shift).astype(jnp.bfloat16)
    velocity = jnp.dot(modulated, head_weight, preferred_element_type=jnp.float32)
    velocity = velocity.reshape(N_WIN, N_FSDP, FW, P_SIZE // N_FSDP, C)
    velocity = jnp.transpose(velocity, (0, 2, 1, 3, 4)).reshape(N_WIN * FW, P_SIZE * C)
    fresh = latents + step_size[0] * velocity
    frames_all = fresh.reshape(N_WIN, FW, P_SIZE * C)
    frame_ids = jnp.arange(FW, dtype=jnp.int32)
    over_prev = jnp.roll(intersections, 1).astype(jnp.int32)
    over_next = intersections.astype(jnp.int32)
    ramp_prev = jnp.roll(ramps, 1, axis=0).astype(jnp.float32)
    ramp_own = ramps.astype(jnp.float32)
    before_win = jnp.roll(frames_all, 1, axis=0)
    after_win = jnp.roll(frames_all, -1, axis=0)
    source_prev = jnp.clip(FW - over_prev[:, None] + frame_ids[None, :], 0, FW - 1).astype(jnp.int32)
    prev_aligned = jnp.take_along_axis(before_win, source_prev[:, :, None], axis=1)
    inside_prev = frame_ids[None, :] < over_prev[:, None]
    prev_index = jnp.minimum(frame_ids, FD - 1).astype(jnp.int32)
    weight_before = ramp_prev[:, prev_index, 0]
    weight_self = ramp_prev[:, prev_index, 1]
    blend_prev = (weight_before[:, :, None] * prev_aligned + weight_self[:, :, None] * frames_all) / (weight_before + weight_self)[:, :, None]
    shifted = frame_ids[None, :] - (FW - over_next[:, None])
    inside_next = shifted >= 0
    source_next = jnp.clip(shifted, 0, FW - 1).astype(jnp.int32)
    next_aligned = jnp.take_along_axis(after_win, source_next[:, :, None], axis=1)
    next_index = jnp.clip(shifted, 0, FD - 1).astype(jnp.int32)
    weight_mine = jnp.take_along_axis(ramp_own[:, :, 0], next_index, axis=1)
    weight_after = jnp.take_along_axis(ramp_own[:, :, 1], next_index, axis=1)
    blend_next = (weight_mine[:, :, None] * frames_all + weight_after[:, :, None] * next_aligned) / (weight_mine + weight_after)[:, :, None]
    blended = jnp.where(inside_prev[:, :, None], blend_prev, jnp.where(inside_next[:, :, None], blend_next, frames_all))
    return blended.reshape(N_WIN * FW, P_SIZE * C)
```

```python
import functools
import math

import jax
import jax.numpy as jnp
from jax import lax
from jax.experimental import pallas as pl
from jax.experimental.pallas import tpu as pltpu
from jax.sharding import PartitionSpec as P

HEADS = 20
HD = 128
FD = 4
EPSILON = 0.001
MESH = pl.DeviceIdType.MESH
F32 = jnp.float32
BF16 = jnp.bfloat16


def kernel(
    ring, n_blk, q_ref, k_ref, v_ref, stream_ref, ow_ref, gate_ref, shift_ref, scale_ref, wt_ref,
    lat_ref, step_ref, inter_ref, ramps_ref, out_ref,
    qkv, attended, weights, residual, side_out, side_in, own_out, own_in, cross_hold, cross_out,
    cross_in, hidden, flat, fresh, before, after,
    qkv_send, qkv_recv, qkv_local, w_send, w_recv, w_local, res_sem, side_send, side_recv,
    own_send, own_recv, cross_send, cross_recv, edge_send, edge_recv,
):
    win, n_win = lax.axis_index("win"), lax.axis_size("win")
    me, groups = lax.axis_index("fsdp"), lax.axis_size("fsdp")
    rows = q_ref.shape[0]
    heads = qkv.shape[1]
    width = weights.shape[2]
    chip, core = me // 2, me % 2
    sibling = chip * 2 + (1 - core)
    far_chip = 1 - chip
    far = far_chip * 2 + core
    far_sibling = far_chip * 2 + (1 - core)
    inputs = (q_ref, k_ref, v_ref)

    up_win, down_win = lax.rem(win + 1, n_win), lax.rem(win + n_win - 1, n_win)
    half_ring = n_win // 2

    def spot_of(w):
        odd = w % 2
        return (1 - odd) * (w // 2) + odd * (n_win - 1 - w // 2)

    def win_of(spot):
        late = spot // half_ring
        return (1 - late) * (2 * spot) + late * (2 * (n_win - 1 - spot) + 1)

    spot = spot_of(win)
    ring_next = win_of(lax.rem(spot + 1, n_win))
    ring_prev = win_of(lax.rem(spot + n_win - 1, n_win))

    if ring:
        blocks = [win]
        for s in range(1, half_ring):
            blocks.append(win_of(lax.rem(spot - s + n_win, n_win)))
            blocks.append(win_of(lax.rem(spot + s, n_win)))
        blocks.append(win_of(lax.rem(spot + half_ring, n_win)))
    else:
        blocks = [jnp.int32(j) for j in range(n_blk)]

    def columns(j):
        return pl.ds(pl.multiple_of(blocks[j] * width, 128), width)

    def qkv_copy(t, h, to, slot):
        return pltpu.make_async_remote_copy(
            src_ref=inputs[t].at[:, pl.ds(pl.multiple_of((to * heads + h) * HD, HD), HD)],
            dst_ref=qkv.at[t, h, pl.ds(pl.multiple_of(me * rows, rows), rows), :],
            send_sem=qkv_send.at[t, h, slot],
            recv_sem=qkv_recv.at[t, h, me],
            device_id={"fsdp": to},
            device_id_type=MESH,
        )

    def qkv_arrival(t, h, source):
        return pltpu.make_async_remote_copy(
            src_ref=inputs[t].at[:, pl.ds(pl.multiple_of((source * heads + h) * HD, HD), HD)],
            dst_ref=qkv.at[t, h, pl.ds(pl.multiple_of(source * rows, rows), rows), :],
            send_sem=qkv_send.at[t, h, 0],
            recv_sem=qkv_recv.at[t, h, source],
            device_id={"fsdp": source},
            device_id_type=MESH,
        )

    def qkv_own(t, h):
        return pltpu.make_async_copy(
            inputs[t].at[:, pl.ds(pl.multiple_of((me * heads + h) * HD, HD), HD)],
            qkv.at[t, h, pl.ds(pl.multiple_of(me * rows, rows), rows), :],
            qkv_local.at[t, h],
        )

    peers = (far, far_sibling, sibling)

    def weight_copy(src, dst, slot, to):
        return pltpu.make_async_remote_copy(
            src_ref=src, dst_ref=dst, send_sem=w_send.at[slot], recv_sem=w_recv.at[slot],
            device_id={"win": to}, device_id_type=MESH,
        )

    depth_half = weights.shape[1] // 2
    last = n_blk - 1

    def forward_copies(s):
        if s < half_ring:
            up_src = ow_ref if s == 1 else weights.at[2 * s - 3]
            down_src = ow_ref if s == 1 else weights.at[2 * s - 2]
            return (
                weight_copy(up_src, weights.at[2 * s - 1], 2 * s - 2, ring_next),
                weight_copy(down_src, weights.at[2 * s], 2 * s - 1, ring_prev),
            )
        top, low = pl.ds(0, depth_half), pl.ds(depth_half, depth_half)
        return (
            weight_copy(weights.at[2 * s - 3, top], weights.at[last, top], 2 * s - 2, ring_next),
            weight_copy(weights.at[2 * s - 2, low], weights.at[last, low], 2 * s - 1, ring_prev),
        )

    def weight_local(j):
        source = ow_ref if ring else ow_ref.at[:, columns(j)]
        return pltpu.make_async_copy(source, weights.at[j], w_local.at[j])

    def residual_copy(j):
        return pltpu.make_async_copy(
            stream_ref.at[:, columns(j)], residual.at[j], res_sem.at[j]
        )

    barrier = pltpu.get_barrier_semaphore()
    for peer in peers:
        pl.semaphore_signal(barrier, inc=1, device_id={"fsdp": peer}, device_id_type=MESH)
    greeted = [up_win, down_win] + ([ring_next, ring_prev] if ring else [])
    for other in greeted:
        pl.semaphore_signal(barrier, inc=1, device_id={"win": other}, device_id_type=MESH)
    pl.semaphore_wait(barrier, len(peers) + len(greeted))

    def start_heads(kinds):
        def start_head(h, carry):
            for t in kinds:
                for slot, peer in enumerate(peers):
                    qkv_copy(t, h, peer, slot).start()
                qkv_own(t, h).start()
            return carry

        lax.fori_loop(0, heads, start_head, 0)

    start_heads((1, 2))
    if ring:
        for copy in forward_copies(1):
            copy.start()
    start_heads((0,))
    for j in range(1 if ring else n_blk):
        weight_local(j).start()
    for j in range(n_blk):
        residual_copy(j).start()

    factor = math.log2(math.e) / math.sqrt(HD)

    def attend(h, first):
        def piece(i, carry):
            at = pl.ds(pl.multiple_of(first + i * rows, rows), rows)
            query = qkv[0, h, at, :]
            scores = lax.dot_general(
                query, qkv[1, h], (((1,), (1,)), ((), ())), preferred_element_type=F32
            )
            highest = jnp.max(scores, axis=-1, keepdims=True)
            exponent = jnp.exp2((scores - highest) * factor)
            denominator = jnp.sum(exponent, axis=-1, keepdims=True)
            summed = jnp.dot(exponent.astype(BF16), qkv[2, h], preferred_element_type=F32)
            attended[at, pl.ds(pl.multiple_of(h * HD, HD), HD)] = (summed / denominator).astype(
                BF16
            )
            return carry

        lax.fori_loop(0, 2, piece, 0)

    def near_head(h, carry):
        for t in (1, 2):
            for source in peers:
                qkv_arrival(t, h, source).wait_recv()
            qkv_own(t, h).wait()
        qkv_arrival(0, h, sibling).wait_recv()
        qkv_own(0, h).wait()
        attend(h, chip * 2 * rows)
        return carry

    lax.fori_loop(0, heads, near_head, 0)
    if ring:
        for copy in forward_copies(1):
            copy.wait_recv()
        for copy in forward_copies(2):
            copy.start()

    def far_head(h, carry):
        for source in (far, far_sibling):
            qkv_arrival(0, h, source).wait_recv()
        attend(h, far_chip * 2 * rows)
        return carry

    lax.fori_loop(0, heads, far_head, 0)

    def part_copy(src, dst, send, recv, j, to):
        return pltpu.make_async_remote_copy(
            src_ref=src.at[j], dst_ref=dst.at[j], send_sem=send.at[j], recv_sem=recv.at[j],
            device_id={"fsdp": to}, device_id_type=MESH,
        )

    def side_copy(j):
        return part_copy(side_out, side_in, side_send, side_recv, j, sibling)

    def own_copy(j):
        return part_copy(own_out, own_in, own_send, own_recv, j, sibling)

    def cross_copy(j):
        return part_copy(cross_out, cross_in, cross_send, cross_recv, j, far)

    def product(group, j):
        at = pl.ds(pl.multiple_of(group * rows, rows), rows)
        return jnp.dot(attended[at, :], weights[j], preferred_element_type=F32)

    for j in range(n_blk):
        if not ring or j == 0:
            weight_local(j).wait()
        elif j % 2 == 1:
            s = (j + 1) // 2
            if s > 1:
                for copy in forward_copies(s):
                    copy.wait_recv()
                if s < half_ring:
                    for copy in forward_copies(s + 1):
                        copy.start()
        side_out[j] = product(far_sibling, j).astype(BF16)
        side_copy(j).start()
        cross_hold[...] = product(far, j)
        own_out[j] = product(sibling, j).astype(BF16)
        own_copy(j).start()
        hidden[j] = product(me, j)
        side_copy(j).wait_recv()
        cross_out[j] = (cross_hold[...] + side_in[j].astype(F32)).astype(BF16)
        cross_copy(j).start()
        residual_copy(j).wait()
        own_copy(j).wait_recv()
        hidden[j] = residual[j].astype(F32) + gate_ref[:, columns(j)] * (
            hidden[j] + own_in[j].astype(F32)
        )

    centres, spreads = [], []
    for j in range(n_blk):
        cross_copy(j).wait_recv()
        block = hidden[j] + gate_ref[:, columns(j)] * cross_in[j].astype(F32)
        hidden[j] = block
        centre = jnp.sum(block, axis=-1, keepdims=True) * (1.0 / width)
        centred = block - centre
        centres.append(centre)
        spreads.append(jnp.sum(centred * centred, axis=-1, keepdims=True))
    mean = functools.reduce(jnp.add, centres) * (1.0 / n_blk)
    spread = functools.reduce(jnp.add, spreads)
    for centre in centres:
        spread = spread + width * (centre - mean) * (centre - mean)
    inverse = 1.0 / jnp.sqrt(spread * (1.0 / (width * n_blk)) + EPSILON)
    velocity = None
    for j in range(n_blk):
        modulated = (
            (hidden[j] - mean) * inverse * scale_ref[:, columns(j)] + shift_ref[:, columns(j)]
        ).astype(BF16)
        term = lax.dot_general(
            modulated, wt_ref[:, columns(j)], (((1,), (1,)), ((), ())), preferred_element_type=F32
        )
        velocity = term if velocity is None else velocity + term

    channels = wt_ref.shape[0]
    frames, wide = lat_ref.shape
    per_frame = wide // channels
    flat[:, :channels] = velocity
    step = step_ref[0]
    for p in range(0, per_frame, 2):
        pair = jnp.concatenate(
            [flat[pl.ds(p + i, frames, stride=per_frame), :][:, :channels] for i in range(2)],
            axis=1,
        )
        at = pl.ds(p * channels, 2 * channels)
        fresh[:, at] = lat_ref[:, at] + step * pair

    edge = before.shape[0]

    def edge_copy(src, dst, slot, to):
        return pltpu.make_async_remote_copy(
            src_ref=src, dst_ref=dst, send_sem=edge_send.at[slot], recv_sem=edge_recv.at[slot],
            device_id={"win": to}, device_id_type=MESH,
        )

    end_rows = pl.ds(frames - edge, edge)
    edges = (
        edge_copy(fresh.at[end_rows], before, 0, up_win),
        edge_copy(fresh.at[pl.ds(0, edge)], after, 1, down_win),
    )
    for copy in edges:
        copy.start()
    if frames > 2 * edge:
        middle = pl.ds(edge, frames - 2 * edge)
        out_ref[middle, :] = fresh[middle, :]
    index = lax.broadcasted_iota(jnp.int32, (edge, 1), 0)
    over_prev, over_next = inter_ref[down_win], inter_ref[win]
    zero = jnp.zeros((edge, 1), jnp.int32)

    def blend(aligned, mine, theirs_w, mine_w):
        theirs = theirs_w.astype(F32)
        own = jnp.where(mine_w > 0, mine_w, 1).astype(F32)
        return (theirs * aligned + own * mine) / (theirs + own)

    for copy in edges:
        copy.wait_recv()

    weight_theirs, weight_own = zero, zero
    for i in range(FD):
        hit = (index == i) & (index < over_prev)
        weight_theirs = jnp.where(hit, ramps_ref[down_win, 2 * i], weight_theirs)
        weight_own = jnp.where(hit, ramps_ref[down_win, 2 * i + 1], weight_own)
    aligned = jnp.zeros((edge, wide), F32)
    chosen = before[...]
    for o in range(1, FD + 1):
        hit = (zero + over_prev) == o
        aligned = jnp.where(hit, pltpu.roll(chosen, o, 0), aligned)
    out_ref[:edge, :] = blend(aligned, fresh[:edge, :], weight_theirs, weight_own)

    weight_theirs, weight_own = zero, zero
    for i in range(FD):
        hit = (index == edge - over_next + i)
        weight_own = jnp.where(hit, ramps_ref[win, 2 * i], weight_own)
        weight_theirs = jnp.where(hit, ramps_ref[win, 2 * i + 1], weight_theirs)
    aligned = jnp.zeros((edge, wide), F32)
    chosen = after[...]
    for o in range(1, FD + 1):
        hit = (zero + over_next) == o
        aligned = jnp.where(hit, pltpu.roll(chosen, edge - o, 0), aligned)
    out_ref[end_rows, :] = blend(aligned, fresh[end_rows, :], weight_theirs, weight_own)

    def finish_head(h, carry):
        for t in range(3):
            for slot, peer in enumerate(peers):
                qkv_copy(t, h, peer, slot).wait_send()
        return carry

    lax.fori_loop(0, heads, finish_head, 0)
    if ring:
        for s in range(1, half_ring + 1):
            for copy in forward_copies(s):
                copy.wait_send()
    for j in range(n_blk):
        side_copy(j).wait_send()
        own_copy(j).wait_send()
        cross_copy(j).wait_send()
    for copy in edges:
        copy.wait_send()


def local(
    queries,
    keys,
    values,
    stream,
    out_weight,
    gate,
    head_shift,
    head_scale,
    head_weight,
    latents,
    step_size,
    intersections,
    ramps,
):
    rows, features = queries.shape
    groups, n_win = lax.axis_size("fsdp"), lax.axis_size("win")
    heads = features // HD // groups
    depth, part = out_weight.shape
    model = stream.shape[1]
    ring = part % 128 == 0 and n_win % 2 == 0 and n_win >= 6
    if ring:
        n_blk, width = n_win, part
    else:
        n_blk = 8
        width = model // n_blk
        out_weight = lax.all_gather(out_weight, "win", axis=1, tiled=True)
    frames, wide = latents.shape
    edge = 8
    any_spec = pl.BlockSpec(memory_space=pl.ANY)
    vmem = pl.BlockSpec(memory_space=pltpu.VMEM)
    smem = pl.BlockSpec(memory_space=pltpu.SMEM)
    dma = pltpu.SemaphoreType.DMA
    parts = pltpu.VMEM((n_blk, rows, width), BF16)
    return pl.pallas_call(
        functools.partial(kernel, ring, n_blk),
        out_shape=jax.ShapeDtypeStruct(latents.shape, latents.dtype),
        in_specs=[any_spec] * 5 + [vmem] * 5 + [smem] * 3,
        out_specs=vmem,
        scratch_shapes=[
            pltpu.VMEM((3, heads, groups * rows, HD), BF16),
            pltpu.VMEM((groups * rows, heads * HD), BF16),
            pltpu.VMEM((n_blk, depth, width), BF16),
            parts, parts, parts, parts, parts,
            pltpu.VMEM((rows, width), F32),
            parts, parts,
            pltpu.VMEM((n_blk, rows, width), F32),
            pltpu.VMEM((rows, 128), F32),
            pltpu.VMEM((frames, wide), F32),
            pltpu.VMEM((edge, wide), F32),
            pltpu.VMEM((edge, wide), F32),
            dma((3, heads, 3)), dma((3, heads, groups)), dma((3, heads)),
            dma((n_blk,)), dma((n_blk,)), dma((n_blk,)), dma((n_blk,)),
            dma((n_blk,)), dma((n_blk,)), dma((n_blk,)), dma((n_blk,)),
            dma((n_blk,)), dma((n_blk,)), dma((2,)), dma((2,)),
        ],
        compiler_params=pltpu.CompilerParams(
            collective_id=0, has_side_effects=True, vmem_limit_bytes=60 * 1024 * 1024
        ),
    )(
        queries, keys, values, stream, out_weight,
        gate[None, :], head_shift[None, :], head_scale[None, :], head_weight.T, latents,
        step_size, intersections, ramps.reshape(n_win, -1),
    )


def solution(mesh):
    in_specs = (
        P(("win", "fsdp"), None),
        P(("win", "fsdp"), None),
        P(("win", "fsdp"), None),
        P(("win", "fsdp"), None),
        P("fsdp", "win"),
        P(),
        P(),
        P(),
        P(),
        P("win", "fsdp"),
        P(),
        P(),
        P(),
    )
    out_specs = P("win", "fsdp")
    return jax.shard_map(local, mesh=mesh, in_specs=in_specs, out_specs=out_specs, check_vma=False)
```

```python
import functools
import math

import jax
import jax.numpy as jnp
from jax import lax
from jax.experimental import pallas as pl
from jax.experimental.pallas import tpu as pltpu
from jax.sharding import PartitionSpec as P

HEADS = 20
HD = 128
FD = 4
EPSILON = 0.001
MESH = pl.DeviceIdType.MESH
F32 = jnp.float32
BF16 = jnp.bfloat16


def kernel(
    ring, n_blk, q_ref, k_ref, v_ref, stream_ref, ow_ref, gate_ref, shift_ref, scale_ref, wt_ref,
    lat_ref, step_ref, inter_ref, ramps_ref, out_ref,
    qkv, attended, weights, residual, side_out, side_in, own_out, own_in, cross_hold, cross_out,
    cross_in, hidden, flat, fresh, before, after, head_rows,
    qkv_send, qkv_recv, qkv_local, w_send, w_recv, w_local, res_sem, side_send, side_recv,
    own_send, own_recv, cross_send, cross_recv, edge_send, edge_recv,
):
    win, n_win = lax.axis_index("win"), lax.axis_size("win")
    me, groups = lax.axis_index("fsdp"), lax.axis_size("fsdp")
    rows = q_ref.shape[0]
    heads = qkv.shape[1]
    width = weights.shape[2]
    chip, core = me // 2, me % 2
    sibling = chip * 2 + (1 - core)
    far_chip = 1 - chip
    far = far_chip * 2 + core
    far_sibling = far_chip * 2 + (1 - core)
    inputs = (q_ref, k_ref, v_ref)

    up_win, down_win = lax.rem(win + 1, n_win), lax.rem(win + n_win - 1, n_win)
    half_ring = n_win // 2

    def spot_of(w):
        odd = w % 2
        return (1 - odd) * (w // 2) + odd * (n_win - 1 - w // 2)

    def win_of(spot):
        late = spot // half_ring
        return (1 - late) * (2 * spot) + late * (2 * (n_win - 1 - spot) + 1)

    spot = spot_of(win)
    ring_next = win_of(lax.rem(spot + 1, n_win))
    ring_prev = win_of(lax.rem(spot + n_win - 1, n_win))

    if ring:
        blocks = [win]
        for s in range(1, half_ring):
            blocks.append(win_of(lax.rem(spot - s + n_win, n_win)))
            blocks.append(win_of(lax.rem(spot + s, n_win)))
        blocks.append(win_of(lax.rem(spot + half_ring, n_win)))
    else:
        blocks = [jnp.int32(j) for j in range(n_blk)]

    def columns(j):
        return pl.ds(pl.multiple_of(blocks[j] * width, 128), width)

    def qkv_copy(t, h, to, slot):
        return pltpu.make_async_remote_copy(
            src_ref=inputs[t].at[:, pl.ds(pl.multiple_of((to * heads + h) * HD, HD), HD)],
            dst_ref=qkv.at[t, h, pl.ds(pl.multiple_of(me * rows, rows), rows), :],
            send_sem=qkv_send.at[t, h, slot],
            recv_sem=qkv_recv.at[t, h, me],
            device_id={"fsdp": to},
            device_id_type=MESH,
        )

    def qkv_arrival(t, h, source):
        return pltpu.make_async_remote_copy(
            src_ref=inputs[t].at[:, pl.ds(pl.multiple_of((source * heads + h) * HD, HD), HD)],
            dst_ref=qkv.at[t, h, pl.ds(pl.multiple_of(source * rows, rows), rows), :],
            send_sem=qkv_send.at[t, h, 0],
            recv_sem=qkv_recv.at[t, h, source],
            device_id={"fsdp": source},
            device_id_type=MESH,
        )

    def qkv_own(t, h):
        return pltpu.make_async_copy(
            inputs[t].at[:, pl.ds(pl.multiple_of((me * heads + h) * HD, HD), HD)],
            qkv.at[t, h, pl.ds(pl.multiple_of(me * rows, rows), rows), :],
            qkv_local.at[t, h],
        )

    peers = (far, far_sibling, sibling)

    def weight_copy(src, dst, slot, to):
        return pltpu.make_async_remote_copy(
            src_ref=src, dst_ref=dst, send_sem=w_send.at[slot], recv_sem=w_recv.at[slot],
            device_id={"win": to}, device_id_type=MESH,
        )

    depth_half = weights.shape[1] // 2
    last = n_blk - 1

    def forward_copies(s):
        if s < half_ring:
            up_src = ow_ref if s == 1 else weights.at[2 * s - 3]
            down_src = ow_ref if s == 1 else weights.at[2 * s - 2]
            return (
                weight_copy(up_src, weights.at[2 * s - 1], 2 * s - 2, ring_next),
                weight_copy(down_src, weights.at[2 * s], 2 * s - 1, ring_prev),
            )
        top, low = pl.ds(0, depth_half), pl.ds(depth_half, depth_half)
        return (
            weight_copy(weights.at[2 * s - 3, top], weights.at[last, top], 2 * s - 2, ring_next),
            weight_copy(weights.at[2 * s - 2, low], weights.at[last, low], 2 * s - 1, ring_prev),
        )

    def weight_local(j):
        source = ow_ref if ring else ow_ref.at[:, columns(j)]
        return pltpu.make_async_copy(source, weights.at[j], w_local.at[j])

    def residual_copy(j):
        return pltpu.make_async_copy(
            stream_ref.at[:, columns(j)], residual.at[j], res_sem.at[j]
        )

    barrier = pltpu.get_barrier_semaphore()
    for peer in peers:
        pl.semaphore_signal(barrier, inc=1, device_id={"fsdp": peer}, device_id_type=MESH)
    greeted = [up_win, down_win] + ([ring_next, ring_prev] if ring else [])
    for other in greeted:
        pl.semaphore_signal(barrier, inc=1, device_id={"win": other}, device_id_type=MESH)
    pl.semaphore_wait(barrier, len(peers) + len(greeted))

    def start_heads(kinds):
        def start_head(h, carry):
            for t in kinds:
                for slot, peer in enumerate(peers):
                    qkv_copy(t, h, peer, slot).start()
                qkv_own(t, h).start()
            return carry

        lax.fori_loop(0, heads, start_head, 0)

    start_heads((1, 2))
    if ring:
        for copy in forward_copies(1):
            copy.start()
    start_heads((0,))
    for j in range(1 if ring else n_blk):
        weight_local(j).start()
    for j in range(n_blk):
        residual_copy(j).start()

    head = wt_ref[...].astype(F32)
    for i, vector in enumerate((scale_ref, shift_ref)):
        head_rows[8 * i : 8 * i + 8] = lax.dot_general(
            jnp.broadcast_to(vector[...], (8, head.shape[1])), head, (((1,), (1,)), ((), ())),
            precision=lax.Precision.HIGHEST, preferred_element_type=F32,
        )

    factor = math.log2(math.e) / math.sqrt(HD)

    def attend(h, first):
        def piece(i, carry):
            at = pl.ds(pl.multiple_of(first + i * rows, rows), rows)
            query = qkv[0, h, at, :]
            scores = lax.dot_general(
                query, qkv[1, h], (((1,), (1,)), ((), ())), preferred_element_type=F32
            )
            highest = jnp.max(scores, axis=-1, keepdims=True)
            exponent = jnp.exp2((scores - highest) * factor)
            denominator = jnp.sum(exponent, axis=-1, keepdims=True)
            summed = jnp.dot(exponent.astype(BF16), qkv[2, h], preferred_element_type=F32)
            attended[at, pl.ds(pl.multiple_of(h * HD, HD), HD)] = (summed / denominator).astype(
                BF16
            )
            return carry

        lax.fori_loop(0, 2, piece, 0)

    def near_head(h, carry):
        for t in (1, 2):
            for source in peers:
                qkv_arrival(t, h, source).wait_recv()
            qkv_own(t, h).wait()
        qkv_arrival(0, h, sibling).wait_recv()
        qkv_own(0, h).wait()
        attend(h, chip * 2 * rows)
        return carry

    lax.fori_loop(0, heads, near_head, 0)
    if ring:
        for copy in forward_copies(1):
            copy.wait_recv()
        for copy in forward_copies(2):
            copy.start()

    def far_head(h, carry):
        for source in (far, far_sibling):
            qkv_arrival(0, h, source).wait_recv()
        attend(h, far_chip * 2 * rows)
        return carry

    lax.fori_loop(0, heads, far_head, 0)

    def part_copy(src, dst, send, recv, j, to):
        return pltpu.make_async_remote_copy(
            src_ref=src.at[j], dst_ref=dst.at[j], send_sem=send.at[j], recv_sem=recv.at[j],
            device_id={"fsdp": to}, device_id_type=MESH,
        )

    def side_copy(j):
        return part_copy(side_out, side_in, side_send, side_recv, j, sibling)

    def own_copy(j):
        return part_copy(own_out, own_in, own_send, own_recv, j, sibling)

    def cross_copy(j):
        return part_copy(cross_out, cross_in, cross_send, cross_recv, j, far)

    def product(group, j):
        at = pl.ds(pl.multiple_of(group * rows, rows), rows)
        return jnp.dot(attended[at, :], weights[j], preferred_element_type=F32)

    for j in range(n_blk):
        if not ring or j == 0:
            weight_local(j).wait()
        elif j % 2 == 1:
            s = (j + 1) // 2
            if s > 1:
                for copy in forward_copies(s):
                    copy.wait_recv()
                if s < half_ring:
                    for copy in forward_copies(s + 1):
                        copy.start()
        side_out[j] = product(far_sibling, j).astype(BF16)
        side_copy(j).start()
        cross_hold[...] = product(far, j)
        own_out[j] = product(sibling, j).astype(BF16)
        own_copy(j).start()
        hidden[j] = product(me, j)
        side_copy(j).wait_recv()
        cross_out[j] = (cross_hold[...] + side_in[j].astype(F32)).astype(BF16)
        cross_copy(j).start()
        residual_copy(j).wait()
        own_copy(j).wait_recv()
        hidden[j] = residual[j].astype(F32) + gate_ref[:, columns(j)] * (
            hidden[j] + own_in[j].astype(F32)
        )

    centres, spreads, raw, pivot = [], [], None, None
    for j in range(n_blk):
        cross_copy(j).wait_recv()
        block = hidden[j] + gate_ref[:, columns(j)] * cross_in[j].astype(F32)
        if j == 0:
            pivot = jnp.sum(block, axis=-1, keepdims=True) * (1.0 / width)
        shifted = block - pivot
        term = lax.dot_general(
            (shifted * scale_ref[:, columns(j)]).astype(BF16), wt_ref[:, columns(j)],
            (((1,), (1,)), ((), ())), preferred_element_type=F32,
        )
        raw = term if raw is None else raw + term
        centre = jnp.sum(shifted, axis=-1, keepdims=True) * (1.0 / width)
        centred = shifted - centre
        centres.append(centre)
        spreads.append(jnp.sum(centred * centred, axis=-1, keepdims=True))
    mean = functools.reduce(jnp.add, centres) * (1.0 / n_blk)
    spread = functools.reduce(jnp.add, spreads)
    for centre in centres:
        spread = spread + width * (centre - mean) * (centre - mean)
    inverse = 1.0 / jnp.sqrt(spread * (1.0 / (width * n_blk)) + EPSILON)
    velocity = inverse * (raw - mean * head_rows[:1]) + head_rows[8:9]

    channels = wt_ref.shape[0]
    frames, wide = lat_ref.shape
    per_frame = wide // channels
    flat[:, :channels] = velocity
    step = step_ref[0]
    for p in range(0, per_frame, 2):
        pair = jnp.concatenate(
            [flat[pl.ds(p + i, frames, stride=per_frame), :][:, :channels] for i in range(2)],
            axis=1,
        )
        at = pl.ds(p * channels, 2 * channels)
        fresh[:, at] = lat_ref[:, at] + step * pair

    edge = before.shape[0]

    def edge_copy(src, dst, slot, to):
        return pltpu.make_async_remote_copy(
            src_ref=src, dst_ref=dst, send_sem=edge_send.at[slot], recv_sem=edge_recv.at[slot],
            device_id={"win": to}, device_id_type=MESH,
        )

    end_rows = pl.ds(frames - edge, edge)
    edges = (
        edge_copy(fresh.at[end_rows], before, 0, up_win),
        edge_copy(fresh.at[pl.ds(0, edge)], after, 1, down_win),
    )
    for copy in edges:
        copy.start()
    if frames > 2 * edge:
        middle = pl.ds(edge, frames - 2 * edge)
        out_ref[middle, :] = fresh[middle, :]
    index = lax.broadcasted_iota(jnp.int32, (edge, 1), 0)
    over_prev, over_next = inter_ref[down_win], inter_ref[win]
    zero = jnp.zeros((edge, 1), jnp.int32)

    def blend(aligned, mine, theirs_w, mine_w):
        theirs = theirs_w.astype(F32)
        own = jnp.where(mine_w > 0, mine_w, 1).astype(F32)
        return (theirs * aligned + own * mine) / (theirs + own)

    for copy in edges:
        copy.wait_recv()

    weight_theirs, weight_own = zero, zero
    for i in range(FD):
        hit = (index == i) & (index < over_prev)
        weight_theirs = jnp.where(hit, ramps_ref[2 * i, down_win], weight_theirs)
        weight_own = jnp.where(hit, ramps_ref[2 * i + 1, down_win], weight_own)
    aligned = jnp.zeros((edge, wide), F32)
    chosen = before[...]
    for o in range(1, FD + 1):
        hit = (zero + over_prev) == o
        aligned = jnp.where(hit, pltpu.roll(chosen, o, 0), aligned)
    out_ref[:edge, :] = blend(aligned, fresh[:edge, :], weight_theirs, weight_own)

    weight_theirs, weight_own = zero, zero
    for i in range(FD):
        hit = (index == edge - over_next + i)
        weight_own = jnp.where(hit, ramps_ref[2 * i, win], weight_own)
        weight_theirs = jnp.where(hit, ramps_ref[2 * i + 1, win], weight_theirs)
    aligned = jnp.zeros((edge, wide), F32)
    chosen = after[...]
    for o in range(1, FD + 1):
        hit = (zero + over_next) == o
        aligned = jnp.where(hit, pltpu.roll(chosen, edge - o, 0), aligned)
    out_ref[end_rows, :] = blend(aligned, fresh[end_rows, :], weight_theirs, weight_own)

    def finish_head(h, carry):
        for t in range(3):
            for slot, peer in enumerate(peers):
                qkv_copy(t, h, peer, slot).wait_send()
        return carry

    lax.fori_loop(0, heads, finish_head, 0)
    if ring:
        for s in range(1, half_ring + 1):
            for copy in forward_copies(s):
                copy.wait_send()
    for j in range(n_blk):
        side_copy(j).wait_send()
        own_copy(j).wait_send()
        cross_copy(j).wait_send()
    for copy in edges:
        copy.wait_send()


def local(
    queries,
    keys,
    values,
    stream,
    out_weight,
    gate,
    head_shift,
    head_scale,
    head_weight,
    latents,
    step_size,
    intersections,
    ramps,
):
    rows, features = queries.shape
    groups, n_win = lax.axis_size("fsdp"), lax.axis_size("win")
    heads = features // HD // groups
    depth, part = out_weight.shape
    model = stream.shape[1]
    ring = part % 128 == 0 and n_win % 2 == 0 and n_win >= 6
    if ring:
        n_blk, width = n_win, part
    else:
        n_blk = 8
        width = model // n_blk
        out_weight = lax.all_gather(out_weight, "win", axis=1, tiled=True)
    frames, wide = latents.shape
    edge = 8
    any_spec = pl.BlockSpec(memory_space=pl.ANY)
    vmem = pl.BlockSpec(memory_space=pltpu.VMEM)
    smem = pl.BlockSpec(memory_space=pltpu.SMEM)
    dma = pltpu.SemaphoreType.DMA
    parts = pltpu.VMEM((n_blk, rows, width), BF16)
    return pl.pallas_call(
        functools.partial(kernel, ring, n_blk),
        out_shape=jax.ShapeDtypeStruct(latents.shape, latents.dtype),
        in_specs=[any_spec] * 5 + [vmem] * 5 + [smem] * 3,
        out_specs=vmem,
        scratch_shapes=[
            pltpu.VMEM((3, heads, groups * rows, HD), BF16),
            pltpu.VMEM((groups * rows, heads * HD), BF16),
            pltpu.VMEM((n_blk, depth, width), BF16),
            parts, parts, parts, parts, parts,
            pltpu.VMEM((rows, width), F32),
            parts, parts,
            pltpu.VMEM((n_blk, rows, width), F32),
            pltpu.VMEM((rows, 128), F32),
            pltpu.VMEM((frames, wide), F32),
            pltpu.VMEM((edge, wide), F32),
            pltpu.VMEM((edge, wide), F32),
            pltpu.VMEM((16, head_weight.shape[1]), F32),
            dma((3, heads, 3)), dma((3, heads, groups)), dma((3, heads)),
            dma((n_blk,)), dma((n_blk,)), dma((n_blk,)), dma((n_blk,)),
            dma((n_blk,)), dma((n_blk,)), dma((n_blk,)), dma((n_blk,)),
            dma((n_blk,)), dma((n_blk,)), dma((2,)), dma((2,)),
        ],
        compiler_params=pltpu.CompilerParams(
            collective_id=0, has_side_effects=True, vmem_limit_bytes=60 * 1024 * 1024
        ),
    )(
        queries, keys, values, stream, out_weight,
        gate[None, :], head_shift[None, :], head_scale[None, :], head_weight.T, latents,
        step_size, intersections, jnp.transpose(ramps, (1, 2, 0)).reshape(-1, n_win),
    )


def solution(mesh):
    in_specs = (
        P(("win", "fsdp"), None),
        P(("win", "fsdp"), None),
        P(("win", "fsdp"), None),
        P(("win", "fsdp"), None),
        P("fsdp", "win"),
        P(),
        P(),
        P(),
        P(),
        P("win", "fsdp"),
        P(),
        P(),
        P(),
    )
    out_specs = P("win", "fsdp")
    return jax.shard_map(local, mesh=mesh, in_specs=in_specs, out_specs=out_specs, check_vma=False)
```
